32 devices in a mesh: dp: 1 (over z), tp: 4 (over y), cp: 8 (over x, core).
Axes of the slice: x: 4, y: 4, z: 1, core: 2. Of those that a mesh axis runs over, the one named last changes fastest.
The devices are a block of a 4x4x8 slice.
Arguments:
- x: bfloat16 [8192, 5376], P(('dp', 'cp', 'tp'))
- w_q: bfloat16 [5376, 4096], P(None, 'tp')
- w_k: bfloat16 [5376, 2048], P(None, 'tp')
- w_v: bfloat16 [5376, 2048], P(None, 'tp')
- w_o: bfloat16 [4096, 5376], P('tp')
Outputs:
- output: bfloat16 [8192, 5376], P(('dp', 'cp', 'tp'))
All inputs are finite; a program needn't handle non-finite values.
Results may differ from the reference program's by a relative error of at most 0.00599733.
Values are sent between devices in bfloat16 or wider.
A program may use at most 768 MiB of HBM per device.

```python
import jax
import jax.numpy as jnp
from jax import lax

D = 5376
HEADS = 32
KV_HEADS = 16
HEAD = 128
SEQ = 8192
CP = 8
Q_BLOCK = 128


def stored_positions():
    piece_len = SEQ // (2 * CP)
    row_idx = jnp.arange(SEQ)
    block_idx = row_idx // (2 * piece_len)
    within = row_idx % (2 * piece_len)
    return jnp.where(within < piece_len, block_idx * piece_len + within, (2 * CP - 1 - block_idx) * piece_len + within - piece_len)


def setup_inputs(seed: int = 0, part: int = 0) -> dict:
    base_key = jax.random.key(seed)
    key_x = jax.random.fold_in(jax.random.fold_in(base_key, 1), part)
    key_q, key_k, key_v, key_o = jax.random.split(jax.random.fold_in(base_key, 2), 4)
    x_val = jax.random.normal(key_x, (SEQ, D), jnp.float32)
    w_q = jax.random.normal(key_q, (D, HEADS * HEAD), jnp.float32) * (1.6 * D ** -0.5)
    w_k = jax.random.normal(key_k, (D, KV_HEADS * HEAD), jnp.float32) * (1.6 * D ** -0.5)
    w_v = jax.random.normal(key_v, (D, KV_HEADS * HEAD), jnp.float32) * (D ** -0.5)
    w_o = jax.random.normal(key_o, (HEADS * HEAD, D), jnp.float32) * (3.0 * (HEADS * HEAD) ** -0.5)
    return {"x": x_val.astype(jnp.bfloat16), "w_q": w_q.astype(jnp.bfloat16), "w_k": w_k.astype(jnp.bfloat16), "w_v": w_v.astype(jnp.bfloat16), "w_o": w_o.astype(jnp.bfloat16)}


def reference(x, w_q, w_k, w_v, w_o):
    group_size = HEADS // KV_HEADS
    score_scale = HEAD ** -0.5
    q_proj = jnp.dot(x, w_q, preferred_element_type=jnp.float32).astype(jnp.bfloat16)
    k_proj = jnp.dot(x, w_k, preferred_element_type=jnp.float32).astype(jnp.bfloat16)
    v_proj = jnp.dot(x, w_v, preferred_element_type=jnp.float32).astype(jnp.bfloat16)
    q_blocks = q_proj.astype(jnp.float32).reshape(SEQ // Q_BLOCK, Q_BLOCK, KV_HEADS, group_size, HEAD)
    k_heads = jnp.transpose(k_proj.astype(jnp.float32).reshape(SEQ, KV_HEADS, HEAD), (1, 0, 2))
    v_heads = jnp.transpose(v_proj.astype(jnp.float32).reshape(SEQ, KV_HEADS, HEAD), (1, 0, 2))
    positions = stored_positions()
    pos_blocks = positions.reshape(SEQ // Q_BLOCK, Q_BLOCK)

    def one_block(block_args):
        q_blk, pos_blk = block_args
        visible = pos_blk[:, None] >= positions[None, :]

        def one_head(head_args):
            q_head, k_head, v_head = head_args
            scores = jnp.einsum("qge,ke->gqk", q_head, k_head) * score_scale
            scores = jnp.where(visible[None], scores, -jnp.inf)
            row_max = scores.max(axis=-1, keepdims=True)
            p_block = jnp.exp(scores - row_max)
            row_sum = p_block.sum(axis=-1)
            weighted = jnp.einsum("gqk,ke->qge", p_block.astype(jnp.bfloat16).astype(jnp.float32), v_head)
            return weighted / jnp.transpose(row_sum)[:, :, None]

        head_outs = lax.map(one_head, (jnp.transpose(q_blk, (1, 0, 2, 3)), k_heads, v_heads))
        return jnp.transpose(head_outs, (1, 0, 2, 3))

    attn_out = lax.map(one_block, (q_blocks, pos_blocks))
    attn_out = attn_out.reshape(SEQ, HEADS * HEAD).astype(jnp.bfloat16)
    return jnp.dot(attn_out, w_o, preferred_element_type=jnp.float32).astype(jnp.bfloat16)
```

```python
import functools
import math

import jax
import jax.numpy as jnp
from jax import lax
from jax.experimental import pallas as pl
from jax.experimental.pallas import tpu as pltpu
from jax.sharding import PartitionSpec as P

HEAD_DIM = 128
F32 = jnp.float32
BF16 = jnp.bfloat16
MESH = pl.DeviceIdType.MESH
SCALE_LOG2 = math.log2(math.e) / math.sqrt(float(HEAD_DIM))
N_TILE = 512
VMEM_LIMIT = 62 * 1024 * 1024


def gather_project_kernel(cp_size, x_ref, wq_ref, wk_ref, wv_ref, q_out, kv_out,
                          x_buf, w_buf, out_buf, load_sem, x_send, x_recv, kv_send, kv_recv, store_sem):
    tp_rank = lax.axis_index("tp")
    cp_rank = lax.axis_index("cp")
    n_tp = 4
    x_rank, core = cp_rank // 2, lax.rem(cp_rank, 2)
    n_x = cp_size // 2
    up_tp, down_tp = lax.rem(tp_rank + 1, n_tp), lax.rem(tp_rank + n_tp - 1, n_tp)
    opp_tp = lax.rem(tp_rank + 2, n_tp)
    up_x, down_x = lax.rem(x_rank + 1, n_x), lax.rem(x_rank + n_x - 1, n_x)
    opp_x = lax.rem(x_rank + 2, n_x)
    up_cp, down_cp, opp_cp = up_x * 2 + core, down_x * 2 + core, opp_x * 2 + core
    partner = x_rank * 2 + 1 - core
    rows = x_ref.shape[0]
    half = rows // 2
    piece = 2 * rows
    n_cols = wk_ref.shape[1]

    loads = [pltpu.make_async_copy(x_ref, x_buf.at[0], load_sem.at[0])]
    w_parts = [(wk_ref, 0), (wv_ref, 0), (wq_ref, 0), (wq_ref, N_TILE)]
    for idx, (ref, col) in enumerate(w_parts):
        loads.append(pltpu.make_async_copy(ref.at[:, pl.ds(col, N_TILE)], w_buf.at[idx], load_sem.at[1 + idx]))
    for copy in loads:
        copy.start()

    barrier = pltpu.get_barrier_semaphore()
    for target in ({"tp": up_tp}, {"tp": down_tp}, {"cp": up_cp}, {"cp": down_cp}, {"cp": partner}):
        pl.semaphore_signal(barrier, inc=1, device_id=target, device_id_type=MESH)
    pl.semaphore_wait(barrier, 5)

    def x_copy(src, stage, part, idx, target):
        return pltpu.make_async_remote_copy(
            src_ref=src, dst_ref=x_buf.at[stage, pl.ds(part * half, half), :],
            send_sem=x_send.at[idx], recv_sem=x_recv.at[idx], device_id={"tp": target}, device_id_type=MESH)

    first, second = x_ref.at[pl.ds(0, half), :], x_ref.at[pl.ds(half, half), :]
    x_copies = [
        x_copy(first, 1, 0, 0, up_tp),
        x_copy(second, 2, 0, 1, up_tp),
        x_copy(second, 1, 1, 2, down_tp),
        x_copy(first, 2, 1, 3, down_tp),
        x_copy(x_buf.at[1, pl.ds(0, half), :], 3, 0, 4, up_tp),
        x_copy(x_buf.at[1, pl.ds(half, half), :], 3, 1, 5, down_tp),
    ]
    x_copies[0].start()
    x_copies[2].start()
    x_copies[1].start()
    x_copies[3].start()

    owners = [
        ((tp_rank, 0), (tp_rank, 1)),
        ((down_tp, 0), (up_tp, 1)),
        ((down_tp, 1), (up_tp, 0)),
        ((opp_tp, 0), (opp_tp, 1)),
    ]

    def kv_rows(cp_owner, stage, part):
        tp_owner, which = owners[stage][part]
        index = jnp.where(tp_owner < 2, cp_owner, 2 * cp_size - 1 - cp_owner)
        row = index * piece + lax.rem(tp_owner, 2) * rows + which * half
        return kv_out.at[pl.ds(pl.multiple_of(row, half), half), :]

    def kv_copy(src, dst, stage, idx, target):
        return pltpu.make_async_remote_copy(
            src_ref=src, dst_ref=dst, send_sem=kv_send.at[stage, idx], recv_sem=kv_recv.at[stage, idx],
            device_id={"cp": target}, device_id_type=MESH)

    def own_kv(stage, part):
        return out_buf.at[stage, pl.ds(part * half, half), pl.ds(0, 2 * n_cols)]

    def kv_sends(stage):
        copies = []
        for part in range(2):
            dst = kv_rows(cp_rank, stage, part)
            copies.append(kv_copy(own_kv(stage, part), dst, stage, part, up_cp))
            copies.append(kv_copy(own_kv(stage, part), dst, stage, 2 + part, down_cp))
            copies.append(kv_copy(own_kv(stage, part), dst, stage, 4 + part, partner))
        return copies

    def kv_forwards(stage):
        below = [kv_rows(down_cp, stage, part) for part in range(2)]
        above = [kv_rows(up_cp, stage, part) for part in range(2)]
        return [
            kv_copy(below[0], below[0], stage, 6, up_cp),
            kv_copy(above[1], above[1], stage, 7, down_cp),
            kv_copy(below[0], below[0], stage, 8, partner),
            kv_copy(above[1], above[1], stage, 9, partner),
            kv_copy(below[1], below[1], stage, 10, partner),
            kv_copy(above[0], above[0], stage, 11, partner),
        ]

    def kv_relays(stage):
        far = [kv_rows(opp_cp, stage, part) for part in range(2)]
        return [kv_copy(far[part], far[part], stage, 12 + part, partner) for part in range(2)]

    stores = []

    def project(stage):
        def tile(idx, carry):
            val = jnp.dot(x_buf[stage], w_buf[idx], preferred_element_type=F32)
            out_buf[stage, :, pl.ds(pl.multiple_of(idx * N_TILE, N_TILE), N_TILE)] = val.astype(BF16)
            return carry

        if stage == 0:
            for idx in range(4):
                loads[1 + idx].wait()
        lax.fori_loop(0, 4, tile, 0)
        for part in range(2):
            tp_owner, which = owners[stage][part]
            row = pl.multiple_of(tp_owner * rows + which * half, half)
            q_store = pltpu.make_async_copy(
                out_buf.at[stage, pl.ds(part * half, half), pl.ds(2 * n_cols, q_out.shape[1])],
                q_out.at[pl.ds(row, half), :], store_sem.at[stage, part])
            kv_store = pltpu.make_async_copy(own_kv(stage, part), kv_rows(cp_rank, stage, part),
                                             store_sem.at[stage, 2 + part])
            for copy in (q_store, kv_store):
                copy.start()
                stores.append(copy)

    sent = []
    for stage in range(4):
        if stage == 0:
            loads[0].wait()
        elif stage == 1:
            x_copies[0].wait_recv()
            x_copies[4].start()
            x_copies[2].wait_recv()
            x_copies[5].start()
        elif stage == 2:
            x_copies[1].wait_recv()
            x_copies[3].wait_recv()
        else:
            x_copies[4].wait_recv()
            x_copies[5].wait_recv()
        project(stage)
        sends = kv_sends(stage)
        for copy in sends:
            copy.start()
        if stage > 0:
            for copy in forwards[:2]:
                copy.wait_recv()
            relays = kv_relays(stage - 1)
            for copy in relays:
                copy.start()
            sent += relays
        forwards = kv_forwards(stage)
        by_idx = {0: sends[0], 2: sends[1], 1: sends[3], 3: sends[4]}
        by_idx[0].wait_recv()
        forwards[0].start()
        by_idx[3].wait_recv()
        forwards[1].start()
        forwards[2].start()
        forwards[3].start()
        by_idx[1].wait_recv()
        forwards[4].start()
        by_idx[2].wait_recv()
        forwards[5].start()
        sent += sends + forwards
    for copy in forwards[:2]:
        copy.wait_recv()
    relays = kv_relays(3)
    for copy in relays:
        copy.start()
    sent += relays
    for stage in range(4):
        arrivals = kv_sends(stage)
        arrivals = [arrivals[2], arrivals[5]] + kv_forwards(stage)[2:] + kv_relays(stage)
        for copy in arrivals:
            copy.wait_recv()
    for copy in sent + x_copies:
        copy.wait_send()
    for copy in stores:
        copy.wait()


def gather_project(x_loc, w_q, w_k, w_v, cp_size):
    rows, width = x_loc.shape
    q_cols, k_cols = w_q.shape[1], w_k.shape[1]
    any_spec = pl.BlockSpec(memory_space=pl.ANY)
    return pl.pallas_call(
        functools.partial(gather_project_kernel, cp_size),
        out_shape=(jax.ShapeDtypeStruct((4 * rows, q_cols), BF16),
                   jax.ShapeDtypeStruct((4 * rows * cp_size, 2 * k_cols), BF16)),
        in_specs=[any_spec] * 4,
        out_specs=(any_spec, any_spec),
        scratch_shapes=[
            pltpu.VMEM((4, rows, width), BF16),
            pltpu.VMEM((4, width, N_TILE), BF16),
            pltpu.VMEM((4, rows, q_cols + 2 * k_cols), BF16),
            pltpu.SemaphoreType.DMA((5,)),
            pltpu.SemaphoreType.DMA((6,)),
            pltpu.SemaphoreType.DMA((6,)),
            pltpu.SemaphoreType.DMA((4, 14)),
            pltpu.SemaphoreType.DMA((4, 14)),
            pltpu.SemaphoreType.DMA((4, 4)),
        ],
        compiler_params=pltpu.CompilerParams(collective_id=0, has_side_effects=True, vmem_limit_bytes=VMEM_LIMIT),
        cost_estimate=pl.CostEstimate(flops=2 * 4 * rows * width * (q_cols + 2 * k_cols), bytes_accessed=80_000_000, transcendentals=0),
        name="gather_project",
    )(x_loc, w_q, w_k, w_v)


def attention_kernel(n_pieces, group, q_chunk, q_ref, k_ref, v_ref, o_ref, acc, run_max, run_sum):
    rank = lax.axis_index("cp")
    piece = q_ref.shape[0] // 2

    def block(which, first, key_row):
        keys = k_ref[pl.ds(key_row, piece), :]
        vals = v_ref[pl.ds(key_row, piece), :]
        chains = [(g, c) for g in range(group) for c in range(piece // q_chunk)]
        scores = []
        for g, c in chains:
            q = q_ref[pl.ds(which * piece + c * q_chunk, q_chunk), g * HEAD_DIM:(g + 1) * HEAD_DIM]
            scores.append(lax.dot_general(q, keys, (((1,), (1,)), ((), ())), preferred_element_type=F32))
        for (g, c), s in zip(chains, scores):
            if first:
                key_pos = lax.broadcasted_iota(jnp.int32, s.shape, 1)
                q_pos = lax.broadcasted_iota(jnp.int32, s.shape, 0) + c * q_chunk
                s = jnp.where(key_pos <= q_pos, s, -jnp.inf)
            sl = slice(c * q_chunk, (c + 1) * q_chunk)
            block_max = jnp.broadcast_to(jnp.max(s, axis=1, keepdims=True) * SCALE_LOG2, (q_chunk, HEAD_DIM))
            if first:
                new_max = block_max
            else:
                old_max = run_max[g, sl, :]
                new_max = jnp.maximum(old_max, block_max)
            p = jnp.exp2(s * SCALE_LOG2 - jnp.concatenate([new_max] * (piece // HEAD_DIM), axis=1))
            sums = p[:, :HEAD_DIM]
            for t in range(1, piece // HEAD_DIM):
                sums = sums + p[:, t * HEAD_DIM:(t + 1) * HEAD_DIM]
            weighted = jnp.dot(p.astype(BF16), vals, preferred_element_type=F32)
            if first:
                run_sum[g, sl, :] = sums
                acc[g, sl, :] = weighted
            else:
                rescale = jnp.exp2(old_max - new_max)
                run_sum[g, sl, :] = run_sum[g, sl, :] * rescale + sums
                acc[g, sl, :] = acc[g, sl, :] * rescale + weighted
            run_max[g, sl, :] = new_max

    for which in range(2):
        index = rank if which == 0 else n_pieces - 1 - rank
        block(which, True, pl.multiple_of(index * piece, piece))

        def body(j, carry):
            block(which, False, pl.multiple_of(j * piece, piece))
            return carry

        lax.fori_loop(0, index, body, 0)
        for g in range(group):
            total = jnp.sum(run_sum[g], axis=1, keepdims=True)
            o_ref[pl.ds(which * piece, piece), g * HEAD_DIM:(g + 1) * HEAD_DIM] = (acc[g] / total).astype(BF16)


def attention(q, kv):
    rows = q.shape[0]
    piece = rows // 2
    kv_heads = kv.shape[1] // (2 * HEAD_DIM)
    group = q.shape[1] // HEAD_DIM // kv_heads
    n_pieces = kv.shape[0] // piece
    return pl.pallas_call(
        functools.partial(attention_kernel, n_pieces, group, piece),
        grid=(kv_heads,),
        in_specs=[pl.BlockSpec((rows, group * HEAD_DIM), lambda h: (0, h)),
                  pl.BlockSpec((kv.shape[0], HEAD_DIM), lambda h: (0, h)),
                  pl.BlockSpec((kv.shape[0], HEAD_DIM), lambda h: (0, kv_heads + h))],
        out_specs=pl.BlockSpec((rows, group * HEAD_DIM), lambda h: (0, h)),
        out_shape=jax.ShapeDtypeStruct(q.shape, BF16),
        scratch_shapes=[pltpu.VMEM((group, piece, HEAD_DIM), F32)] * 3,
        compiler_params=pltpu.CompilerParams(vmem_limit_bytes=48 * 1024 * 1024),
        cost_estimate=pl.CostEstimate(flops=40_000_000_000, bytes_accessed=22_000_000, transcendentals=36_000_000),
        name="attention",
    )(q, kv, kv)


def solution(mesh):
    cp_size = mesh.shape["cp"]
    row_spec = P(("dp", "cp", "tp"), None)

    def local_layer(x_loc, w_q, w_k, w_v, w_o):
        q, kv = gather_project(x_loc, w_q, w_k, w_v, cp_size)
        share = w_o.shape[0] // cp_size
        w_slice = lax.dynamic_slice_in_dim(w_o, lax.axis_index("cp") * share, share, axis=0)
        w_slice, kv = lax.optimization_barrier((w_slice, kv))
        w_full = lax.all_gather(w_slice, ("tp", "cp"), axis=0, tiled=True)
        attn = attention(q, kv)
        attn_rows = lax.all_to_all(attn, "tp", split_axis=0, concat_axis=1, tiled=True)
        return jnp.dot(attn_rows, w_full, preferred_element_type=F32).astype(BF16)

    return jax.shard_map(local_layer, mesh=mesh, in_specs=(row_spec, P(None, "tp"), P(None, "tp"), P(None, "tp"), P("tp", None)), out_specs=row_spec, check_vma=False)
```

```python
import functools
import math

import jax
import jax.numpy as jnp
from jax import lax
from jax.experimental import pallas as pl
from jax.experimental.pallas import tpu as pltpu
from jax.sharding import PartitionSpec as P

HEAD_DIM = 128
F32 = jnp.float32
BF16 = jnp.bfloat16
MESH = pl.DeviceIdType.MESH
SCALE_LOG2 = math.log2(math.e) / math.sqrt(float(HEAD_DIM))
N_TILE = 512
VMEM_LIMIT = 62 * 1024 * 1024


def wo_window(parity, which, core, rows, cols):
    row = pl.multiple_of(parity * (rows // 2) + which * (rows // 4), rows // 4)
    col = pl.multiple_of(core * (cols // 2), HEAD_DIM)
    return pl.ds(row, rows // 4), pl.ds(col, cols // 2)


def tp_block_copy(wo_ref, wo_out, rel, which, target, send_sem, recv_sem):
    cp_rank = lax.axis_index("cp")
    window = wo_window(lax.rem(cp_rank // 2, 2), which, lax.rem(cp_rank, 2), *wo_ref.shape)
    return pltpu.make_async_remote_copy(
        src_ref=wo_ref.at[window], dst_ref=wo_out.at[(rel,) + window], send_sem=send_sem, recv_sem=recv_sem,
        device_id={"tp": target}, device_id_type=MESH)


def gather_project_kernel(cp_size, x_ref, wq_ref, wk_ref, wv_ref, wo_ref, q_out, kv_out, wo_out,
                          x_buf, w_buf, out_buf, load_sem, x_send, x_recv, kv_send, kv_recv, store_sem, wo_send, wo_recv):
    tp_rank = lax.axis_index("tp")
    cp_rank = lax.axis_index("cp")
    n_tp = 4
    x_rank, core = cp_rank // 2, lax.rem(cp_rank, 2)
    n_x = cp_size // 2
    up_tp, down_tp = lax.rem(tp_rank + 1, n_tp), lax.rem(tp_rank + n_tp - 1, n_tp)
    opp_tp = lax.rem(tp_rank + 2, n_tp)
    up_x, down_x = lax.rem(x_rank + 1, n_x), lax.rem(x_rank + n_x - 1, n_x)
    opp_x = lax.rem(x_rank + 2, n_x)
    up_cp, down_cp, opp_cp = up_x * 2 + core, down_x * 2 + core, opp_x * 2 + core
    partner = x_rank * 2 + 1 - core
    rows = x_ref.shape[0]
    half = rows // 2
    piece = 2 * rows
    n_cols = wk_ref.shape[1]

    loads = [pltpu.make_async_copy(x_ref, x_buf.at[0], load_sem.at[0])]
    w_parts = [(wk_ref, 0), (wv_ref, 0), (wq_ref, 0), (wq_ref, N_TILE)]
    for idx, (ref, col) in enumerate(w_parts):
        loads.append(pltpu.make_async_copy(ref.at[:, pl.ds(col, N_TILE)], w_buf.at[idx], load_sem.at[1 + idx]))
    for copy in loads:
        copy.start()

    barrier = pltpu.get_barrier_semaphore()
    for target in ({"tp": up_tp}, {"tp": down_tp}, {"cp": up_cp}, {"cp": down_cp}, {"cp": partner}):
        pl.semaphore_signal(barrier, inc=1, device_id=target, device_id_type=MESH)
    pl.semaphore_wait(barrier, 5)

    def x_copy(src, stage, part, idx, target):
        return pltpu.make_async_remote_copy(
            src_ref=src, dst_ref=x_buf.at[stage, pl.ds(part * half, half), :],
            send_sem=x_send.at[idx], recv_sem=x_recv.at[idx], device_id={"tp": target}, device_id_type=MESH)

    first, second = x_ref.at[pl.ds(0, half), :], x_ref.at[pl.ds(half, half), :]
    x_copies = [
        x_copy(first, 1, 0, 0, up_tp),
        x_copy(second, 2, 0, 1, up_tp),
        x_copy(second, 1, 1, 2, down_tp),
        x_copy(first, 2, 1, 3, down_tp),
        x_copy(x_buf.at[1, pl.ds(0, half), :], 3, 0, 4, up_tp),
        x_copy(x_buf.at[1, pl.ds(half, half), :], 3, 1, 5, down_tp),
    ]
    x_copies[0].start()
    x_copies[2].start()
    x_copies[1].start()
    x_copies[3].start()

    owners = [
        ((tp_rank, 0), (tp_rank, 1)),
        ((down_tp, 0), (up_tp, 1)),
        ((down_tp, 1), (up_tp, 0)),
        ((opp_tp, 0), (opp_tp, 1)),
    ]

    def kv_rows(cp_owner, stage, part):
        tp_owner, which = owners[stage][part]
        index = jnp.where(tp_owner < 2, cp_owner, 2 * cp_size - 1 - cp_owner)
        row = index * piece + lax.rem(tp_owner, 2) * rows + which * half
        return kv_out.at[pl.ds(pl.multiple_of(row, half), half), :]

    def kv_copy(src, dst, stage, idx, target):
        return pltpu.make_async_remote_copy(
            src_ref=src, dst_ref=dst, send_sem=kv_send.at[stage, idx], recv_sem=kv_recv.at[stage, idx],
            device_id={"cp": target}, device_id_type=MESH)

    def own_kv(stage, part):
        return out_buf.at[stage, pl.ds(part * half, half), pl.ds(0, 2 * n_cols)]

    def kv_sends(stage):
        copies = []
        for part in range(2):
            dst = kv_rows(cp_rank, stage, part)
            copies.append(kv_copy(own_kv(stage, part), dst, stage, part, up_cp))
            copies.append(kv_copy(own_kv(stage, part), dst, stage, 2 + part, down_cp))
            copies.append(kv_copy(own_kv(stage, part), dst, stage, 4 + part, partner))
        return copies

    def kv_forwards(stage):
        below = [kv_rows(down_cp, stage, part) for part in range(2)]
        above = [kv_rows(up_cp, stage, part) for part in range(2)]
        return [
            kv_copy(below[0], below[0], stage, 6, up_cp),
            kv_copy(above[1], above[1], stage, 7, down_cp),
            kv_copy(below[0], below[0], stage, 8, partner),
            kv_copy(above[1], above[1], stage, 9, partner),
            kv_copy(below[1], below[1], stage, 10, partner),
            kv_copy(above[0], above[0], stage, 11, partner),
        ]

    def kv_relays(stage):
        far = [kv_rows(opp_cp, stage, part) for part in range(2)]
        return [kv_copy(far[part], far[part], stage, 12 + part, partner) for part in range(2)]

    stores = []

    def project(stage):
        def tile(idx, carry):
            val = jnp.dot(x_buf[stage], w_buf[idx], preferred_element_type=F32)
            out_buf[stage, :, pl.ds(pl.multiple_of(idx * N_TILE, N_TILE), N_TILE)] = val.astype(BF16)
            return carry

        if stage == 0:
            for idx in range(4):
                loads[1 + idx].wait()
        lax.fori_loop(0, 4, tile, 0)
        for part in range(2):
            tp_owner, which = owners[stage][part]
            row = pl.multiple_of(tp_owner * rows + which * half, half)
            q_store = pltpu.make_async_copy(
                out_buf.at[stage, pl.ds(part * half, half), pl.ds(2 * n_cols, q_out.shape[1])],
                q_out.at[pl.ds(row, half), :], store_sem.at[stage, part])
            kv_store = pltpu.make_async_copy(own_kv(stage, part), kv_rows(cp_rank, stage, part),
                                             store_sem.at[stage, 2 + part])
            for copy in (q_store, kv_store):
                copy.start()
                stores.append(copy)

    sent = []
    for stage in range(4):
        if stage == 0:
            loads[0].wait()
        elif stage == 1:
            x_copies[0].wait_recv()
            x_copies[4].start()
            x_copies[2].wait_recv()
            x_copies[5].start()
        elif stage == 2:
            x_copies[1].wait_recv()
            x_copies[3].wait_recv()
        else:
            x_copies[4].wait_recv()
            x_copies[5].wait_recv()
            wo_copies = [
                tp_block_copy(wo_ref, wo_out, 0, 0, up_tp, wo_send.at[0], wo_recv.at[0]),
                tp_block_copy(wo_ref, wo_out, 1, 1, down_tp, wo_send.at[1], wo_recv.at[1]),
            ]
            for copy in wo_copies:
                copy.start()
        project(stage)
        sends = kv_sends(stage)
        for copy in sends:
            copy.start()
        if stage > 0:
            for copy in forwards[:2]:
                copy.wait_recv()
            relays = kv_relays(stage - 1)
            for copy in relays:
                copy.start()
            sent += relays
        forwards = kv_forwards(stage)
        by_idx = {0: sends[0], 2: sends[1], 1: sends[3], 3: sends[4]}
        by_idx[0].wait_recv()
        forwards[0].start()
        by_idx[3].wait_recv()
        forwards[1].start()
        forwards[2].start()
        forwards[3].start()
        by_idx[1].wait_recv()
        forwards[4].start()
        by_idx[2].wait_recv()
        forwards[5].start()
        sent += sends + forwards
    for copy in forwards[:2]:
        copy.wait_recv()
    relays = kv_relays(3)
    for copy in relays:
        copy.start()
    sent += relays
    for stage in range(4):
        arrivals = kv_sends(stage)
        arrivals = [arrivals[2], arrivals[5]] + kv_forwards(stage)[2:] + kv_relays(stage)
        for copy in arrivals:
            copy.wait_recv()
    for copy in wo_copies:
        copy.wait_recv()
    for copy in sent + x_copies + wo_copies:
        copy.wait_send()
    for copy in stores:
        copy.wait()


def gather_project(x_loc, w_q, w_k, w_v, w_o, cp_size):
    rows, width = x_loc.shape
    q_cols, k_cols = w_q.shape[1], w_k.shape[1]
    any_spec = pl.BlockSpec(memory_space=pl.ANY)
    return pl.pallas_call(
        functools.partial(gather_project_kernel, cp_size),
        out_shape=(jax.ShapeDtypeStruct((4 * rows, q_cols), BF16),
                   jax.ShapeDtypeStruct((4 * rows * cp_size, 2 * k_cols), BF16),
                   jax.ShapeDtypeStruct((3,) + w_o.shape, BF16)),
        in_specs=[any_spec] * 5,
        out_specs=(any_spec, any_spec, any_spec),
        scratch_shapes=[
            pltpu.VMEM((4, rows, width), BF16),
            pltpu.VMEM((4, width, N_TILE), BF16),
            pltpu.VMEM((4, rows, q_cols + 2 * k_cols), BF16),
            pltpu.SemaphoreType.DMA((5,)),
            pltpu.SemaphoreType.DMA((6,)),
            pltpu.SemaphoreType.DMA((6,)),
            pltpu.SemaphoreType.DMA((4, 14)),
            pltpu.SemaphoreType.DMA((4, 14)),
            pltpu.SemaphoreType.DMA((4, 4)),
            pltpu.SemaphoreType.DMA((2,)),
            pltpu.SemaphoreType.DMA((2,)),
        ],
        compiler_params=pltpu.CompilerParams(collective_id=0, has_side_effects=True, vmem_limit_bytes=VMEM_LIMIT),
        cost_estimate=pl.CostEstimate(flops=2 * 4 * rows * width * (q_cols + 2 * k_cols), bytes_accessed=80_000_000, transcendentals=0),
        name="gather_project",
    )(x_loc, w_q, w_k, w_v, w_o)


def attention_kernel(n_pieces, group, q_chunk, cp_size, q_ref, k_ref, v_ref, wo_ref, wo_in, own_out, far_out, wo_out,
                     acc, run_max, run_sum, o_buf, y_send, y_recv, x_send, x_recv, d_send, d_recv, o_send, o_recv, o_local):
    del wo_in
    head = pl.program_id(0)
    n_heads = o_buf.shape[0]
    tp_rank, rank = lax.axis_index("tp"), lax.axis_index("cp")
    x_rank, core = rank // 2, lax.rem(rank, 2)
    n_x = cp_size // 2
    parity = lax.rem(x_rank, 2)
    up_tp, down_tp, opp_tp = (lax.rem(tp_rank + d, 4) for d in (1, 3, 2))
    up_cp = lax.rem(x_rank + 1, n_x) * 2 + core
    down_cp = lax.rem(x_rank + n_x - 1, n_x) * 2 + core
    partner = x_rank * 2 + 1 - core
    piece = q_ref.shape[0] // 2
    rows = q_ref.shape[0] // 4
    width = q_ref.shape[1]

    def wo_block(rel, which, from_cp):
        side = 1 - parity if from_cp else parity
        return wo_out.at[(rel,) + wo_window(side, which, core, *wo_ref.shape)]

    def forward(which):
        return pltpu.make_async_remote_copy(
            src_ref=wo_block(which, which, False), dst_ref=wo_block(2, which, False),
            send_sem=y_send.at[which], recv_sem=y_recv.at[which],
            device_id={"tp": up_tp if which == 0 else down_tp}, device_id_type=MESH)

    def second(rel):
        return tp_block_copy(wo_ref, wo_out, rel, 1 - rel, up_tp if rel == 0 else down_tp,
                             y_send.at[2 + rel], y_recv.at[2 + rel])

    def across(rel, which):
        block = wo_block(rel, which, False)
        return pltpu.make_async_remote_copy(
            src_ref=block, dst_ref=block, send_sem=x_send.at[rel, which], recv_sem=x_recv.at[rel, which],
            device_id={"cp": up_cp if which == 0 else down_cp}, device_id_type=MESH)

    def relay(rel, which, from_cp):
        block = wo_block(rel, which, from_cp)
        slot = int(from_cp)
        return pltpu.make_async_remote_copy(
            src_ref=block, dst_ref=block, send_sem=d_send.at[slot, rel, which], recv_sem=d_recv.at[slot, rel, which],
            device_id={"cp": partner}, device_id_type=MESH)

    def result_copies(h):
        copies = []
        for rel, target in ((0, up_tp), (1, down_tp), (2, opp_tp)):
            copies.append(pltpu.make_async_remote_copy(
                src_ref=o_buf.at[h, pl.ds(pl.multiple_of(target * rows, rows), rows), :],
                dst_ref=far_out.at[rel, :, pl.ds(h * width, width)],
                send_sem=o_send.at[h, rel], recv_sem=o_recv.at[h, rel],
                device_id={"tp": target}, device_id_type=MESH))
        local = pltpu.make_async_copy(o_buf.at[h, pl.ds(pl.multiple_of(tp_rank * rows, rows), rows), :],
                                      own_out.at[:, pl.ds(h * width, width)], o_local.at[h])
        return copies, local

    def send_result(h):
        copies, local = result_copies(h)
        for copy in copies + [local]:
            copy.start()

    def pass_on(rel, which):
        across(rel, which).start()
        relay(rel, which, False).start()

    def relay_across(rel, which):
        across(rel, which).wait_recv()
        relay(rel, which, True).start()

    @pl.when(head == 0)
    def _():
        barrier = pltpu.get_barrier_semaphore()
        for target in ({"tp": up_tp}, {"tp": down_tp}, {"tp": opp_tp}, {"cp": up_cp}, {"cp": down_cp}, {"cp": partner}):
            pl.semaphore_signal(barrier, inc=1, device_id=target, device_id_type=MESH)
        pl.semaphore_wait(barrier, 6)
        forward(0).start()
        forward(1).start()
        second(0).start()
        second(1).start()
        pass_on(0, 0)
        pass_on(1, 1)

    @pl.when(head == 1)
    def _():
        send_result(0)

    @pl.when(head == 2)
    def _():
        for which in range(2):
            forward(which).wait_recv()
            pass_on(2, which)
        relay_across(0, 0)
        relay_across(1, 1)
        send_result(1)

    @pl.when(head == 3)
    def _():
        send_result(2)

    def block(which, first, key_row):
        keys = k_ref[pl.ds(key_row, piece), :]
        vals = v_ref[pl.ds(key_row, piece), :]
        chains = [(g, c) for g in range(group) for c in range(piece // q_chunk)]
        scores = []
        for g, c in chains:
            q = q_ref[pl.ds(which * piece + c * q_chunk, q_chunk), g * HEAD_DIM:(g + 1) * HEAD_DIM]
            scores.append(lax.dot_general(q, keys, (((1,), (1,)), ((), ())), preferred_element_type=F32))
        for (g, c), s in zip(chains, scores):
            if first:
                key_pos = lax.broadcasted_iota(jnp.int32, s.shape, 1)
                q_pos = lax.broadcasted_iota(jnp.int32, s.shape, 0) + c * q_chunk
                s = jnp.where(key_pos <= q_pos, s, -jnp.inf)
            sl = slice(c * q_chunk, (c + 1) * q_chunk)
            block_max = jnp.broadcast_to(jnp.max(s, axis=1, keepdims=True) * SCALE_LOG2, (q_chunk, HEAD_DIM))
            if first:
                new_max = block_max
            else:
                old_max = run_max[g, sl, :]
                new_max = jnp.maximum(old_max, block_max)
            p = jnp.exp2(s * SCALE_LOG2 - jnp.concatenate([new_max] * (piece // HEAD_DIM), axis=1))
            sums = p[:, :HEAD_DIM]
            for t in range(1, piece // HEAD_DIM):
                sums = sums + p[:, t * HEAD_DIM:(t + 1) * HEAD_DIM]
            weighted = jnp.dot(p.astype(BF16), vals, preferred_element_type=F32)
            if first:
                run_sum[g, sl, :] = sums
                acc[g, sl, :] = weighted
            else:
                rescale = jnp.exp2(old_max - new_max)
                run_sum[g, sl, :] = run_sum[g, sl, :] * rescale + sums
                acc[g, sl, :] = acc[g, sl, :] * rescale + weighted
            run_max[g, sl, :] = new_max

    for which in range(2):
        index = rank if which == 0 else n_pieces - 1 - rank
        block(which, True, pl.multiple_of(index * piece, piece))

        def body(j, carry):
            block(which, False, pl.multiple_of(j * piece, piece))
            return carry

        lax.fori_loop(0, index, body, 0)
        for g in range(group):
            total = jnp.sum(run_sum[g], axis=1, keepdims=True)
            o_buf[head, which * piece:(which + 1) * piece, g * HEAD_DIM:(g + 1) * HEAD_DIM] = (acc[g] / total).astype(BF16)

    @pl.when(head == n_heads - 1)
    def _():
        for rel in range(2):
            second(rel).wait_recv()
            pass_on(rel, 1 - rel)
        send_result(n_heads - 1)
        relay_across(2, 0)
        relay_across(2, 1)
        relay_across(0, 1)
        relay_across(1, 0)
        for rel in range(3):
            for which in range(2):
                for from_cp in (False, True):
                    relay(rel, which, from_cp).wait()
                across(rel, which).wait_send()
        for which in range(2):
            forward(which).wait_send()
            second(which).wait_send()
        for h in range(n_heads):
            copies, local = result_copies(h)
            for copy in copies + [local]:
                copy.wait()


def attention(q, kv, w_o, w_far, cp_size):
    rows = q.shape[0]
    piece = rows // 2
    kv_heads = kv.shape[1] // (2 * HEAD_DIM)
    group = q.shape[1] // HEAD_DIM // kv_heads
    n_pieces = kv.shape[0] // piece
    any_spec = pl.BlockSpec(memory_space=pl.ANY)
    dma = pltpu.SemaphoreType.DMA
    return pl.pallas_call(
        functools.partial(attention_kernel, n_pieces, group, piece, cp_size),
        grid=(kv_heads,),
        in_specs=[pl.BlockSpec((rows, group * HEAD_DIM), lambda h: (0, h)),
                  pl.BlockSpec((kv.shape[0], HEAD_DIM), lambda h: (0, h)),
                  pl.BlockSpec((kv.shape[0], HEAD_DIM), lambda h: (0, kv_heads + h)),
                  any_spec, any_spec],
        out_specs=(any_spec, any_spec, any_spec),
        out_shape=(jax.ShapeDtypeStruct((rows // 4, q.shape[1]), BF16),
                   jax.ShapeDtypeStruct((3, rows // 4, q.shape[1]), BF16),
                   jax.ShapeDtypeStruct(w_far.shape, BF16)),
        scratch_shapes=[pltpu.VMEM((group, piece, HEAD_DIM), F32)] * 3 + [
            pltpu.VMEM((kv_heads, rows, group * HEAD_DIM), BF16),
            dma((4,)), dma((4,)), dma((3, 2)), dma((3, 2)), dma((2, 3, 2)), dma((2, 3, 2)),
            dma((kv_heads, 3)), dma((kv_heads, 3)), dma((kv_heads,)),
        ],
        input_output_aliases={4: 2},
        compiler_params=pltpu.CompilerParams(collective_id=1, has_side_effects=True, vmem_limit_bytes=48 * 1024 * 1024,
                                             dimension_semantics=("arbitrary",)),
        cost_estimate=pl.CostEstimate(flops=40_000_000_000, bytes_accessed=22_000_000, transcendentals=36_000_000),
        name="attention",
    )(q, kv, kv, w_o, w_far)


def output_kernel(own_ref, far_ref, wo_ref, w_far_ref, y_ref):
    total = jnp.dot(own_ref[...], wo_ref[...], preferred_element_type=F32)
    for rel in range(3):
        total = total + jnp.dot(far_ref[rel], w_far_ref[rel], preferred_element_type=F32)
    y_ref[...] = total.astype(BF16)


def output_project(own, far, w_o, w_far):
    rows, depth = own.shape
    width = w_o.shape[1]
    tile = 768
    return pl.pallas_call(
        output_kernel,
        grid=(width // tile,),
        in_specs=[pl.BlockSpec((rows, depth), lambda n: (0, 0)),
                  pl.BlockSpec((3, rows, depth), lambda n: (0, 0, 0)),
                  pl.BlockSpec((depth, tile), lambda n: (0, n)),
                  pl.BlockSpec((3, depth, tile), lambda n: (0, 0, n))],
        out_specs=pl.BlockSpec((rows, tile), lambda n: (0, n)),
        out_shape=jax.ShapeDtypeStruct((rows, width), BF16),
        compiler_params=pltpu.CompilerParams(vmem_limit_bytes=48 * 1024 * 1024),
        cost_estimate=pl.CostEstimate(flops=8 * rows * depth * width, bytes_accessed=8 * depth * width, transcendentals=0),
        name="output_project",
    )(own, far, w_o, w_far)


def solution(mesh):
    cp_size = mesh.shape["cp"]
    row_spec = P(("dp", "cp", "tp"), None)

    def local_layer(x_loc, w_q, w_k, w_v, w_o):
        q, kv, w_far = gather_project(x_loc, w_q, w_k, w_v, w_o, cp_size)
        own, far, w_far = attention(q, kv, w_o, w_far, cp_size)
        return output_project(own, far, w_o, w_far)

    return jax.shard_map(local_layer, mesh=mesh, in_specs=(row_spec, P(None, "tp"), P(None, "tp"), P(None, "tp"), P("tp", None)), out_specs=row_spec, check_vma=False)
```

```python
import functools
import math

import jax
import jax.numpy as jnp
from jax import lax
from jax.experimental import pallas as pl
from jax.experimental.pallas import tpu as pltpu
from jax.sharding import PartitionSpec as P

HEAD_DIM = 128
F32 = jnp.float32
BF16 = jnp.bfloat16
MESH = pl.DeviceIdType.MESH
SCALE_LOG2 = math.log2(math.e) / math.sqrt(float(HEAD_DIM))
N_TILE = 512
VMEM_LIMIT = 62 * 1024 * 1024


def wo_window(parity, which, core, rows, cols):
    row = pl.multiple_of(parity * (rows // 2) + which * (rows // 4), rows // 4)
    col = pl.multiple_of(core * (cols // 2), HEAD_DIM)
    return pl.ds(row, rows // 4), pl.ds(col, cols // 2)


def tp_block_copy(wo_ref, wo_out, rel, which, target, send_sem, recv_sem):
    cp_rank = lax.axis_index("cp")
    window = wo_window(lax.rem(cp_rank // 2, 2), which, lax.rem(cp_rank, 2), *wo_ref.shape)
    return pltpu.make_async_remote_copy(
        src_ref=wo_ref.at[window], dst_ref=wo_out.at[(rel,) + window], send_sem=send_sem, recv_sem=recv_sem,
        device_id={"tp": target}, device_id_type=MESH)


def gather_project_kernel(cp_size, x_ref, wq_ref, wk_ref, wv_ref, wo_ref, q_out, kv_out, wo_out,
                          x_buf, w_buf, out_buf, load_sem, x_send, x_recv, kv_send, kv_recv, store_sem, wo_send, wo_recv):
    tp_rank = lax.axis_index("tp")
    cp_rank = lax.axis_index("cp")
    n_tp = 4
    x_rank, core = cp_rank // 2, lax.rem(cp_rank, 2)
    n_x = cp_size // 2
    up_tp, down_tp = lax.rem(tp_rank + 1, n_tp), lax.rem(tp_rank + n_tp - 1, n_tp)
    opp_tp = lax.rem(tp_rank + 2, n_tp)
    up_x, down_x = lax.rem(x_rank + 1, n_x), lax.rem(x_rank + n_x - 1, n_x)
    opp_x = lax.rem(x_rank + 2, n_x)
    up_cp, down_cp, opp_cp = up_x * 2 + core, down_x * 2 + core, opp_x * 2 + core
    partner = x_rank * 2 + 1 - core
    rows = x_ref.shape[0]
    half = rows // 2
    piece = 2 * rows
    n_cols = wk_ref.shape[1]

    loads = [pltpu.make_async_copy(x_ref, x_buf.at[0], load_sem.at[0])]
    w_parts = [(wk_ref, 0), (wv_ref, 0), (wq_ref, 0), (wq_ref, N_TILE)]
    for idx, (ref, col) in enumerate(w_parts):
        loads.append(pltpu.make_async_copy(ref.at[:, pl.ds(col, N_TILE)], w_buf.at[idx], load_sem.at[1 + idx]))
    for copy in loads:
        copy.start()

    barrier = pltpu.get_barrier_semaphore()
    for target in ({"tp": up_tp}, {"tp": down_tp}, {"cp": up_cp}, {"cp": down_cp}, {"cp": partner}):
        pl.semaphore_signal(barrier, inc=1, device_id=target, device_id_type=MESH)
    pl.semaphore_wait(barrier, 5)

    def x_copy(src, stage, part, idx, target):
        return pltpu.make_async_remote_copy(
            src_ref=src, dst_ref=x_buf.at[stage, pl.ds(part * half, half), :],
            send_sem=x_send.at[idx], recv_sem=x_recv.at[idx], device_id={"tp": target}, device_id_type=MESH)

    first, second = x_ref.at[pl.ds(0, half), :], x_ref.at[pl.ds(half, half), :]
    x_copies = [
        x_copy(first, 1, 0, 0, up_tp),
        x_copy(second, 2, 0, 1, up_tp),
        x_copy(second, 1, 1, 2, down_tp),
        x_copy(first, 2, 1, 3, down_tp),
        x_copy(x_buf.at[1, pl.ds(0, half), :], 3, 0, 4, up_tp),
        x_copy(x_buf.at[1, pl.ds(half, half), :], 3, 1, 5, down_tp),
    ]
    x_copies[0].start()
    x_copies[2].start()
    x_copies[1].start()
    x_copies[3].start()

    owners = [
        ((tp_rank, 0), (tp_rank, 1)),
        ((down_tp, 0), (up_tp, 1)),
        ((down_tp, 1), (up_tp, 0)),
        ((opp_tp, 0), (opp_tp, 1)),
    ]

    def kv_rows(cp_owner, stage, part):
        tp_owner, which = owners[stage][part]
        index = jnp.where(tp_owner < 2, cp_owner, 2 * cp_size - 1 - cp_owner)
        row = index * piece + lax.rem(tp_owner, 2) * rows + which * half
        return kv_out.at[pl.ds(pl.multiple_of(row, half), half), :]

    def kv_copy(src, dst, stage, idx, target):
        return pltpu.make_async_remote_copy(
            src_ref=src, dst_ref=dst, send_sem=kv_send.at[stage, idx], recv_sem=kv_recv.at[stage, idx],
            device_id={"cp": target}, device_id_type=MESH)

    def own_kv(stage, part):
        return out_buf.at[stage, pl.ds(part * half, half), pl.ds(0, 2 * n_cols)]

    def kv_sends(stage):
        copies = []
        for part in range(2):
            dst = kv_rows(cp_rank, stage, part)
            copies.append(kv_copy(own_kv(stage, part), dst, stage, part, up_cp))
            copies.append(kv_copy(own_kv(stage, part), dst, stage, 2 + part, down_cp))
            copies.append(kv_copy(own_kv(stage, part), dst, stage, 4 + part, partner))
        return copies

    def kv_forwards(stage):
        below = [kv_rows(down_cp, stage, part) for part in range(2)]
        above = [kv_rows(up_cp, stage, part) for part in range(2)]
        return [
            kv_copy(below[0], below[0], stage, 6, up_cp),
            kv_copy(above[1], above[1], stage, 7, down_cp),
            kv_copy(below[0], below[0], stage, 8, partner),
            kv_copy(above[1], above[1], stage, 9, partner),
            kv_copy(below[1], below[1], stage, 10, partner),
            kv_copy(above[0], above[0], stage, 11, partner),
        ]

    def kv_relays(stage):
        far = [kv_rows(opp_cp, stage, part) for part in range(2)]
        return [kv_copy(far[part], far[part], stage, 12 + part, partner) for part in range(2)]

    stores = []

    def project(stage):
        def tile(idx, carry):
            val = jnp.dot(x_buf[stage], w_buf[idx], preferred_element_type=F32)
            out_buf[stage, :, pl.ds(pl.multiple_of(idx * N_TILE, N_TILE), N_TILE)] = val.astype(BF16)
            return carry

        if stage == 0:
            for idx in range(4):
                loads[1 + idx].wait()
        lax.fori_loop(0, 3, tile, 0)
        sends = kv_sends(stage)
        for copy in sends:
            copy.start()
        lax.fori_loop(3, 4, tile, 0)
        for part in range(2):
            tp_owner, which = owners[stage][part]
            row = pl.multiple_of(tp_owner * rows + which * half, half)
            q_store = pltpu.make_async_copy(
                out_buf.at[stage, pl.ds(part * half, half), pl.ds(2 * n_cols, q_out.shape[1])],
                q_out.at[pl.ds(row, half), :], store_sem.at[stage, part])
            kv_store = pltpu.make_async_copy(own_kv(stage, part), kv_rows(cp_rank, stage, part),
                                             store_sem.at[stage, 2 + part])
            for copy in (q_store, kv_store):
                copy.start()
                stores.append(copy)
        return sends

    sent = []
    for stage in range(4):
        if stage == 0:
            loads[0].wait()
        elif stage == 1:
            x_copies[0].wait_recv()
            x_copies[4].start()
            x_copies[2].wait_recv()
            x_copies[5].start()
        elif stage == 2:
            x_copies[1].wait_recv()
            x_copies[3].wait_recv()
            wo_copies = [
                tp_block_copy(wo_ref, wo_out, 0, 0, up_tp, wo_send.at[0], wo_recv.at[0]),
                tp_block_copy(wo_ref, wo_out, 1, 1, down_tp, wo_send.at[1], wo_recv.at[1]),
            ]
            for copy in wo_copies:
                copy.start()
        else:
            x_copies[4].wait_recv()
            x_copies[5].wait_recv()
        sends = project(stage)
        if stage > 0:
            for copy in forwards[:2]:
                copy.wait_recv()
            relays = kv_relays(stage - 1)
            for copy in relays:
                copy.start()
            sent += relays
        forwards = kv_forwards(stage)
        by_idx = {0: sends[0], 2: sends[1], 1: sends[3], 3: sends[4]}
        by_idx[0].wait_recv()
        forwards[0].start()
        by_idx[3].wait_recv()
        forwards[1].start()
        forwards[2].start()
        forwards[3].start()
        by_idx[1].wait_recv()
        forwards[4].start()
        by_idx[2].wait_recv()
        forwards[5].start()
        sent += sends + forwards
    for copy in forwards[:2]:
        copy.wait_recv()
    relays = kv_relays(3)
    for copy in relays:
        copy.start()
    sent += relays
    for stage in range(4):
        arrivals = kv_sends(stage)
        arrivals = [arrivals[2], arrivals[5]] + kv_forwards(stage)[2:] + kv_relays(stage)
        for copy in arrivals:
            copy.wait_recv()
    for copy in wo_copies:
        copy.wait_recv()
    for copy in sent + x_copies + wo_copies:
        copy.wait_send()
    for copy in stores:
        copy.wait()


def gather_project(x_loc, w_q, w_k, w_v, w_o, cp_size):
    rows, width = x_loc.shape
    q_cols, k_cols = w_q.shape[1], w_k.shape[1]
    any_spec = pl.BlockSpec(memory_space=pl.ANY)
    return pl.pallas_call(
        functools.partial(gather_project_kernel, cp_size),
        out_shape=(jax.ShapeDtypeStruct((4 * rows, q_cols), BF16),
                   jax.ShapeDtypeStruct((4 * rows * cp_size, 2 * k_cols), BF16),
                   jax.ShapeDtypeStruct((3,) + w_o.shape, BF16)),
        in_specs=[any_spec] * 5,
        out_specs=(any_spec, any_spec, any_spec),
        scratch_shapes=[
            pltpu.VMEM((4, rows, width), BF16),
            pltpu.VMEM((4, width, N_TILE), BF16),
            pltpu.VMEM((4, rows, q_cols + 2 * k_cols), BF16),
            pltpu.SemaphoreType.DMA((5,)),
            pltpu.SemaphoreType.DMA((6,)),
            pltpu.SemaphoreType.DMA((6,)),
            pltpu.SemaphoreType.DMA((4, 14)),
            pltpu.SemaphoreType.DMA((4, 14)),
            pltpu.SemaphoreType.DMA((4, 4)),
            pltpu.SemaphoreType.DMA((2,)),
            pltpu.SemaphoreType.DMA((2,)),
        ],
        compiler_params=pltpu.CompilerParams(collective_id=0, has_side_effects=True, vmem_limit_bytes=VMEM_LIMIT),
        cost_estimate=pl.CostEstimate(flops=2 * 4 * rows * width * (q_cols + 2 * k_cols), bytes_accessed=80_000_000, transcendentals=0),
        name="gather_project",
    )(x_loc, w_q, w_k, w_v, w_o)


def attention_kernel(n_pieces, group, q_chunk, cp_size, q_ref, k_ref, v_ref, wo_ref, wo_in, y_ref, wo_out,
                     acc, run_max, run_sum, o_buf, far_buf, y_acc, w_slots,
                     y_send, y_recv, x_send, x_recv, d_send, d_recv, o_send, o_recv, w_load):
    del wo_in
    head = pl.program_id(0)
    n_heads = o_buf.shape[0]
    tp_rank, rank = lax.axis_index("tp"), lax.axis_index("cp")
    x_rank, core = rank // 2, lax.rem(rank, 2)
    n_x = cp_size // 2
    parity = lax.rem(x_rank, 2)
    up_tp, down_tp, opp_tp = (lax.rem(tp_rank + d, 4) for d in (1, 3, 2))
    up_cp = lax.rem(x_rank + 1, n_x) * 2 + core
    down_cp = lax.rem(x_rank + n_x - 1, n_x) * 2 + core
    partner = x_rank * 2 + 1 - core
    piece = q_ref.shape[0] // 2
    rows = q_ref.shape[0] // 4
    width = q_ref.shape[1]

    def wo_block(rel, which, from_cp):
        side = 1 - parity if from_cp else parity
        return wo_out.at[(rel,) + wo_window(side, which, core, *wo_ref.shape)]

    def forward(which):
        return pltpu.make_async_remote_copy(
            src_ref=wo_block(which, which, False), dst_ref=wo_block(2, which, False),
            send_sem=y_send.at[which], recv_sem=y_recv.at[which],
            device_id={"tp": up_tp if which == 0 else down_tp}, device_id_type=MESH)

    def second(rel):
        return tp_block_copy(wo_ref, wo_out, rel, 1 - rel, up_tp if rel == 0 else down_tp,
                             y_send.at[2 + rel], y_recv.at[2 + rel])

    def across(rel, which):
        block = wo_block(rel, which, False)
        return pltpu.make_async_remote_copy(
            src_ref=block, dst_ref=block, send_sem=x_send.at[rel, which], recv_sem=x_recv.at[rel, which],
            device_id={"cp": up_cp if which == 0 else down_cp}, device_id_type=MESH)

    def relay(rel, which, from_cp):
        block = wo_block(rel, which, from_cp)
        slot = int(from_cp)
        return pltpu.make_async_remote_copy(
            src_ref=block, dst_ref=block, send_sem=d_send.at[slot, rel, which], recv_sem=d_recv.at[slot, rel, which],
            device_id={"cp": partner}, device_id_type=MESH)

    def result_copies(h):
        copies = []
        for rel, target in ((0, up_tp), (1, down_tp), (2, opp_tp)):
            copies.append(pltpu.make_async_remote_copy(
                src_ref=o_buf.at[h, pl.ds(pl.multiple_of(target * rows, rows), rows), :],
                dst_ref=far_buf.at[rel, :, pl.ds(h * width, width)],
                send_sem=o_send.at[h, rel], recv_sem=o_recv.at[h, rel],
                device_id={"tp": target}, device_id_type=MESH))
        return copies

    def send_result(h):
        for copy in result_copies(h):
            copy.start()

    def pass_on(rel, which):
        across(rel, which).start()
        relay(rel, which, False).start()

    def relay_across(rel, which):
        across(rel, which).wait_recv()
        relay(rel, which, True).start()

    @pl.when(head == 0)
    def _():
        barrier = pltpu.get_barrier_semaphore()
        for target in ({"tp": up_tp}, {"tp": down_tp}, {"tp": opp_tp}, {"cp": up_cp}, {"cp": down_cp}, {"cp": partner}):
            pl.semaphore_signal(barrier, inc=1, device_id=target, device_id_type=MESH)
        pl.semaphore_wait(barrier, 6)
        forward(0).start()
        forward(1).start()
        second(0).start()
        second(1).start()
        pass_on(0, 0)
        pass_on(1, 1)

    @pl.when(head == 1)
    def _():
        send_result(0)

    @pl.when(head == 2)
    def _():
        for which in range(2):
            forward(which).wait_recv()
            pass_on(2, which)
        relay_across(0, 0)
        relay_across(1, 1)
        send_result(1)

    @pl.when(head == 3)
    def _():
        send_result(2)

    def block(which, first, key_row):
        keys = k_ref[pl.ds(key_row, piece), :]
        vals = v_ref[pl.ds(key_row, piece), :]
        chains = [(g, c) for g in range(group) for c in range(piece // q_chunk)]
        scores = []
        for g, c in chains:
            q = q_ref[pl.ds(which * piece + c * q_chunk, q_chunk), g * HEAD_DIM:(g + 1) * HEAD_DIM]
            scores.append(lax.dot_general(q, keys, (((1,), (1,)), ((), ())), preferred_element_type=F32))
        for (g, c), s in zip(chains, scores):
            if first:
                key_pos = lax.broadcasted_iota(jnp.int32, s.shape, 1)
                q_pos = lax.broadcasted_iota(jnp.int32, s.shape, 0) + c * q_chunk
                s = jnp.where(key_pos <= q_pos, s, -jnp.inf)
            sl = slice(c * q_chunk, (c + 1) * q_chunk)
            block_max = jnp.broadcast_to(jnp.max(s, axis=1, keepdims=True) * SCALE_LOG2, (q_chunk, HEAD_DIM))
            if first:
                new_max = block_max
            else:
                old_max = run_max[g, sl, :]
                new_max = jnp.maximum(old_max, block_max)
            p = jnp.exp2(s * SCALE_LOG2 - jnp.concatenate([new_max] * (piece // HEAD_DIM), axis=1))
            sums = p[:, :HEAD_DIM]
            for t in range(1, piece // HEAD_DIM):
                sums = sums + p[:, t * HEAD_DIM:(t + 1) * HEAD_DIM]
            weighted = jnp.dot(p.astype(BF16), vals, preferred_element_type=F32)
            if first:
                run_sum[g, sl, :] = sums
                acc[g, sl, :] = weighted
            else:
                rescale = jnp.exp2(old_max - new_max)
                run_sum[g, sl, :] = run_sum[g, sl, :] * rescale + sums
                acc[g, sl, :] = acc[g, sl, :] * rescale + weighted
            run_max[g, sl, :] = new_max

    for which in range(2):
        index = rank if which == 0 else n_pieces - 1 - rank
        block(which, True, pl.multiple_of(index * piece, piece))

        def body(j, carry):
            block(which, False, pl.multiple_of(j * piece, piece))
            return carry

        lax.fori_loop(0, index, body, 0)
        for g in range(group):
            total = jnp.sum(run_sum[g], axis=1, keepdims=True)
            o_buf[head, which * piece:(which + 1) * piece, g * HEAD_DIM:(g + 1) * HEAD_DIM] = (acc[g] / total).astype(BF16)

    quarter = wo_ref.shape[0] // 4
    near, beyond = parity * 2 * quarter, (1 - parity) * 2 * quarter
    own_rows = pl.ds(pl.multiple_of(tp_rank * rows, rows), rows)
    chunks = [
        ((None, 0), (None, quarter)),
        ((None, 2 * quarter), (None, 3 * quarter)),
        ((0, near), (0, near + quarter)),
        ((1, near), (1, near + quarter)),
        ((2, near), (2, near + quarter)),
        ((2, beyond), (2, beyond + quarter)),
        ((0, beyond), (1, beyond + quarter)),
        ((0, beyond + quarter), (1, beyond)),
    ]

    def chunk_loads(idx):
        slot = idx % 4
        loads = []
        for part, (rel, row) in enumerate(chunks[idx]):
            window = pl.ds(pl.multiple_of(row, quarter), quarter)
            src = wo_ref.at[window, :] if rel is None else wo_out.at[rel, window, :]
            loads.append(pltpu.make_async_copy(src, w_slots.at[slot, pl.ds(part * quarter, quarter), :],
                                               w_load.at[slot, part]))
        return loads

    def start_loads(idx):
        for copy in chunk_loads(idx):
            copy.start()

    def project(*indices):
        halves = []
        for idx in indices:
            for copy in chunk_loads(idx):
                copy.wait()
            for rel, row in chunks[idx]:
                if rel is None:
                    halves.append(o_buf[row // width, own_rows, :])
                else:
                    halves.append(far_buf[rel, :, pl.ds(pl.multiple_of(row, quarter), quarter)])
        lhs = jnp.concatenate(halves, axis=1)
        tile = 1792
        slot = indices[0] % 4

        def step(n, carry):
            cols = pl.ds(pl.multiple_of(n * tile, tile), tile)
            rhs = w_slots[slot:slot + len(indices), :, cols].reshape(lhs.shape[1], tile)
            val = jnp.dot(lhs, rhs, preferred_element_type=F32)
            if indices[0] > 0:
                val = y_acc[:, cols] + val
            if indices[-1] < len(chunks) - 1:
                y_acc[:, cols] = val
            else:
                y_ref[:, cols] = val.astype(BF16)
            return carry

        lax.fori_loop(0, y_ref.shape[1] // tile, step, 0)

    @pl.when(head == n_heads - 1)
    def _():
        start_loads(0)
        start_loads(1)
        for rel in range(2):
            second(rel).wait_recv()
            pass_on(rel, 1 - rel)
        send_result(n_heads - 1)
        relay_across(2, 0)
        relay_across(2, 1)
        project(0, 1)
        for rel in range(3):
            for which in range(2):
                relay(rel, which, False).wait_recv()
                if rel == 2 or which == rel:
                    relay(rel, which, True).wait_recv()
        for idx in range(2, 6):
            start_loads(idx)
        for h in range(n_heads):
            for copy in result_copies(h):
                copy.wait_recv()
        project(2, 3)
        start_loads(6)
        project(4, 5)
        project(6)
        relay_across(0, 1)
        relay_across(1, 0)
        relay(0, 1, True).wait_recv()
        relay(1, 0, True).wait_recv()
        start_loads(7)
        project(7)
        for rel in range(3):
            for which in range(2):
                for from_cp in (False, True):
                    relay(rel, which, from_cp).wait_send()
                across(rel, which).wait_send()
        for which in range(2):
            forward(which).wait_send()
            second(which).wait_send()
        for h in range(n_heads):
            for copy in result_copies(h):
                copy.wait_send()


def attention(q, kv, w_o, w_far, cp_size):
    rows = q.shape[0]
    piece = rows // 2
    kv_heads = kv.shape[1] // (2 * HEAD_DIM)
    group = q.shape[1] // HEAD_DIM // kv_heads
    n_pieces = kv.shape[0] // piece
    any_spec = pl.BlockSpec(memory_space=pl.ANY)
    dma = pltpu.SemaphoreType.DMA
    return pl.pallas_call(
        functools.partial(attention_kernel, n_pieces, group, piece, cp_size),
        grid=(kv_heads,),
        in_specs=[pl.BlockSpec((rows, group * HEAD_DIM), lambda h: (0, h)),
                  pl.BlockSpec((kv.shape[0], HEAD_DIM), lambda h: (0, h)),
                  pl.BlockSpec((kv.shape[0], HEAD_DIM), lambda h: (0, kv_heads + h)),
                  any_spec, any_spec],
        out_specs=(pl.BlockSpec((rows // 4, w_o.shape[1]), lambda h: (0, 0)), any_spec),
        out_shape=(jax.ShapeDtypeStruct((rows // 4, w_o.shape[1]), BF16), jax.ShapeDtypeStruct(w_far.shape, BF16)),
        scratch_shapes=[pltpu.VMEM((group, piece, HEAD_DIM), F32)] * 3 + [
            pltpu.VMEM((kv_heads, rows, group * HEAD_DIM), BF16),
            pltpu.VMEM((3, rows // 4, q.shape[1]), BF16),
            pltpu.VMEM((rows // 4, w_o.shape[1]), F32),
            pltpu.VMEM((4, w_o.shape[0] // 2, w_o.shape[1]), BF16),
            dma((4,)), dma((4,)), dma((3, 2)), dma((3, 2)), dma((2, 3, 2)), dma((2, 3, 2)),
            dma((kv_heads, 3)), dma((kv_heads, 3)), dma((4, 2)),
        ],
        input_output_aliases={4: 1},
        compiler_params=pltpu.CompilerParams(collective_id=1, has_side_effects=True, vmem_limit_bytes=VMEM_LIMIT,
                                             dimension_semantics=("arbitrary",)),
        cost_estimate=pl.CostEstimate(flops=40_000_000_000, bytes_accessed=22_000_000, transcendentals=36_000_000),
        name="attention",
    )(q, kv, kv, w_o, w_far)


def solution(mesh):
    cp_size = mesh.shape["cp"]
    row_spec = P(("dp", "cp", "tp"), None)

    def local_layer(x_loc, w_q, w_k, w_v, w_o):
        q, kv, w_far = gather_project(x_loc, w_q, w_k, w_v, w_o, cp_size)
        return attention(q, kv, w_o, w_far, cp_size)[0]

    return jax.shard_map(local_layer, mesh=mesh, in_specs=(row_spec, P(None, "tp"), P(None, "tp"), P(None, "tp"), P("tp", None)), out_specs=row_spec, check_vma=False)
```
